512 devices in a mesh: dp: 32 (over z, core), mp: 16 (over y, x).
Axes of the slice: x: 4, y: 4, z: 16, core: 2. Of those that a mesh axis runs over, the one named last changes fastest.
Arguments:
- token_ids: int32 [32768], P('dp'), may hold values from 0 to 128255
- lengths: int32 [256], P('dp'), may hold values from 1 to 128
- embed_grads: bfloat16 [32768, 4096], P('dp', 'mp'), may hold values from -6 to 6
- vocab_basis: bfloat16 [128256, 32], P('mp'), may hold values from -6 to 6
- embed_basis: bfloat16 [4096, 32], P('mp'), may hold values from -0.09375 to 0.09375
- layer_inputs: bfloat16 [1, 32768, 4096], P(None, 'dp', 'mp'), may hold values from -6 to 6
- layer_grads: bfloat16 [1, 32768, 4096], P(None, 'dp', 'mp'), may hold values from -6 to 6
- input_basis: bfloat16 [1, 4096, 32], P(None, 'mp'), may hold values from -0.09375 to 0.09375
- output_basis: bfloat16 [1, 4096, 32], P(None, 'mp'), may hold values from -0.09375 to 0.09375
- queries: bfloat16 [2, 1024, 256], P(None, 'mp', 'dp'), may hold values from -0.19921875 to 0.19921875
Outputs:
- scores: float32 [256, 256], P('dp')
The draws below stay inside these ranges and needn't reach their ends.
All inputs are finite; a program needn't handle non-finite values.
Results may differ from the reference program's by a relative error of at most 0.0003.
Values may be sent and summed in bfloat16 or wider, within the bound.
A program may use at most 64 MiB of HBM per device.

```python
import math
import jax
import jax.numpy as jnp
import numpy as np
from jax import lax

D = 4096
VOCAB = 128256
RANK = 32
LIN = 1
SLOT = 128
QUERIES = 256
ITERS = 2
NL = 2
SK = 1024
TOKENS = 32768
EXAMPLES = 256


def set_ends(entries, stream_key, smallest, largest):
    extent = entries.shape
    index_at = [jax.random.randint(jax.random.fold_in(stream_key, axis), (), 0, extent[axis]) for axis in range(len(extent))]
    entries = entries.at[tuple(index_at)].set(smallest)
    longest = extent.index(max(extent))
    index_at[longest] = (index_at[longest] + 1) % extent[longest]
    return entries.at[tuple(index_at)].set(largest)


def block_scale(rng, extent, pieces, low, top_value):
    def one(dim, blocks):
        draws = jax.random.uniform(jax.random.fold_in(jax.random.fold_in(rng, 6), dim), (blocks,), jnp.float32, low / len(pieces), top_value / len(pieces))
        return jnp.repeat(jnp.exp(draws), extent[dim] // blocks).reshape((-1,) + (1,) * (len(extent) - dim - 1))

    loudness = one(*pieces[0])
    for cut in pieces[1:]:
        loudness = loudness * one(*cut)
    return loudness


def ranked_wide(rng, extent, number_of, skew):
    weights = [min(1 << octave, number_of + 1 - (1 << octave)) * (1 << 20) // math.isqrt((1 << octave) ** skew) + 1 for octave in range((number_of + 1).bit_length()) if 1 << octave <= number_of]
    scale = 1 + sum(weights) // (1 << 30)
    listing = np.cumsum(np.array([max(1, weight // scale) for weight in weights]))
    ticket = jax.random.randint(jax.random.fold_in(rng, 1), extent, 0, int(listing[len(weights) - 1]))
    start = jnp.left_shift(1, jnp.searchsorted(jnp.asarray(listing, jnp.int32), ticket, side="right").astype(jnp.int32))
    rank = start - 1 + jax.random.randint(jax.random.fold_in(rng, 4), extent, 0, 1 << 30) % jnp.minimum(start, number_of + 1 - start)
    return jax.random.permutation(jax.random.fold_in(rng, 2), number_of)[rank].astype(jnp.int32)


def normal_values(own_key, shape, scale, bound, pieces=(), kind=jnp.bfloat16):
    gain = block_scale(own_key, shape, pieces, -0.22, 0.18) if pieces else 1.0
    array = jax.random.normal(own_key, shape, jnp.float32) * scale * gain
    return jnp.minimum(jnp.maximum(array, -bound), bound).astype(kind)


def setup_inputs(seed: int = 0) -> dict:
    splits = jax.random.split(jax.random.key(seed), 11)
    token_ids = set_ends(ranked_wide(splits[0], (TOKENS,), VOCAB, 2), jax.random.fold_in(splits[0], 3), 0, VOCAB - 1).astype(jnp.int32)
    lengths = set_ends(jax.random.randint(splits[1], (EXAMPLES,), 1, SLOT + 1), jax.random.fold_in(splits[1], 1), 1, SLOT).astype(jnp.int32)
    embed_grads = normal_values(splits[2], (TOKENS, D), 1.0, 6.0, ((0, 32), (1, 16)))
    vocab_basis = normal_values(splits[3], (VOCAB, RANK), 1.0, 6.0, ((0, 16),))
    embed_basis = normal_values(splits[4], (D, RANK), D ** -0.5, 0.09375, ((0, 16),))
    layer_inputs = normal_values(splits[5], (LIN, TOKENS, D), 1.0, 6.0, ((1, 32), (2, 16)))
    layer_grads = normal_values(splits[6], (LIN, TOKENS, D), 1.0, 6.0, ((1, 32), (2, 16)))
    input_basis = normal_values(splits[7], (LIN, D, RANK), D ** -0.5, 0.09375, ((1, 16),))
    output_basis = normal_values(splits[8], (LIN, D, RANK), D ** -0.5, 0.09375, ((1, 16),))
    queries = normal_values(splits[9], (NL, SK, QUERIES), 0.03, 0.19921875, ((1, 16), (2, 32)))
    return {"token_ids": token_ids, "lengths": lengths, "embed_grads": embed_grads, "vocab_basis": vocab_basis, "embed_basis": embed_basis, "layer_inputs": layer_inputs, "layer_grads": layer_grads, "input_basis": input_basis, "output_basis": output_basis, "queries": queries}


damping = 0.01
epsilon = 1e-6
highest = lax.Precision.HIGHEST


def solve_columns(gram_mat, right_side, count):
    solution = jnp.zeros_like(right_side)
    residual = right_side
    direction = right_side
    norm_now = jnp.sum(residual * residual, axis=0)
    for iteration in range(ITERS):
        images = jnp.dot(gram_mat, direction, precision=highest) / count + damping * direction
        step_size = norm_now / (jnp.sum(direction * images, axis=0) + epsilon)
        solution = solution + step_size * direction
        residual = residual - step_size * images
        norm_next = jnp.sum(residual * residual, axis=0)
        direction = residual + (norm_next / (norm_now + epsilon)) * direction
        norm_now = norm_next
    return solution


def reference(token_ids, lengths, embed_grads, vocab_basis, embed_basis, layer_inputs, layer_grads, input_basis, output_basis, queries):
    pairs = [(jnp.dot(embed_grads, embed_basis, preferred_element_type=jnp.float32),
              vocab_basis[token_ids].astype(jnp.float32))]
    for layer_idx in range(LIN):
        pairs.append((jnp.dot(layer_grads[layer_idx], output_basis[layer_idx], preferred_element_type=jnp.float32),
                      jnp.dot(layer_inputs[layer_idx], input_basis[layer_idx], preferred_element_type=jnp.float32)))
    inverse_len = 1.0 / lengths.astype(jnp.float32)
    position = jnp.arange(SLOT, dtype=jnp.int32)
    weights = jnp.where(position[None, :] < lengths[:, None], inverse_len[:, None], jnp.float32(0.0))
    scores = jnp.zeros((EXAMPLES, QUERIES), jnp.float32)
    for layer_idx in range(NL):
        grads_proj, inputs_proj = pairs[layer_idx]
        weighted = grads_proj.reshape(EXAMPLES, SLOT, RANK) * weights[:, :, None]
        sketches = jnp.einsum('sti,stj->sij', weighted, inputs_proj.reshape(EXAMPLES, SLOT, RANK),
                              precision=highest).reshape(EXAMPLES, RANK * RANK)
        gram_mat = jnp.dot(sketches.T, sketches, precision=highest)
        solution = solve_columns(gram_mat, queries[layer_idx].astype(jnp.float32), EXAMPLES)
        scores = scores + jnp.dot(sketches, solution, precision=highest)
    return scores
```

```python
import functools

import jax
import jax.numpy as jnp
from jax import lax
from jax.experimental import pallas as pl
from jax.experimental.pallas import tpu as pltpu
from jax.sharding import PartitionSpec as P

DAMPING = 0.01
EPSILON = 1e-06
MESH = pl.DeviceIdType.MESH
F32 = jnp.float32
BF16 = jnp.bfloat16

ZS = 16
MS = 16
REACH = 4
OWN = 7
BLK = 512


def dot_t(a, b):
    return lax.dot_general(a, b, (((1,), (1,)), ((), ())), preferred_element_type=F32)


def dot_n(a, b):
    return lax.dot_general(a, b, (((1,), (0,)), ((), ())), preferred_element_type=F32)


def halves(a):
    high = a.astype(BF16)
    return high, (a - high.astype(F32)).astype(BF16)


def kernel(
    ids_hbm, len_hbm, g0_hbm, vt_hbm, we_hbm, x1_hbm, g1_hbm, wi_hbm, wo_hbm, q_hbm,
    out_ref,
    ids, lens, g0, vt, we, x1, g1, wi, wo, q,
    last, table, send, recv, sk, qz, qg, sg, bt, bb, sh, sl, part, other,
    in_sem, a_send, a_recv, qz_send, qz_recv, qp_send, qp_recv, qs_send, qs_recv,
    sz_send, sz_recv, sp_send, sp_recv, ss_send, ss_recv, c_send, c_recv,
):
    d = lax.axis_index("dp")
    m = lax.axis_index("mp")
    core = d % 2
    z = d // 2
    x = m % 4
    layer = x // 2
    row = (m // 4) * 2 + x % 2
    sibling = (d + 1 - 2 * core, m)
    partner = (d, m - x + 3 - x)

    def along_z(offset):
        return (2 * ((z + offset + ZS) % ZS) + core, m)

    def in_plane(r):
        return (d, (m + r) % MS)

    def group_row(r):
        return (row + r) % 8

    def in_group(r):
        there = group_row(r)
        return (d, (there // 2) * 4 + 2 * layer + there % 2)

    pairs = [
        (ids_hbm, ids), (vt_hbm, vt), (q_hbm, q), (we_hbm, we), (g0_hbm, g0), (wo_hbm, wo),
        (g1_hbm, g1), (wi_hbm, wi), (x1_hbm, x1), (len_hbm, lens),
    ]
    loads = {}
    for n, (src, dst) in enumerate(pairs):
        loads[n] = pltpu.make_async_copy(src, dst, in_sem.at[n])
        loads[n].start()

    barrier = pltpu.get_barrier_semaphore()
    z_offsets = [o for k in range(1, REACH + 1) for o in (k, -k)]
    peers = [in_plane(r) for r in range(1, MS)] + [along_z(o) for o in z_offsets] + [sibling]
    for peer in peers:
        pl.semaphore_signal(barrier, inc=1, device_id=peer, device_id_type=MESH)

    def remote(src, dst, send_sem, recv_sem, peer):
        return pltpu.make_async_remote_copy(
            src_ref=src, dst_ref=dst, send_sem=send_sem, recv_sem=recv_sem,
            device_id=peer, device_id_type=MESH,
        )

    sent = []

    def go(copy):
        copy.start()
        sent.append(copy)

    loads[0].wait()
    loads[1].wait()
    full = vt.shape[1] // BLK
    rest = vt.shape[1] - full * BLK
    last[...] = jnp.zeros(last.shape, BF16)
    last[:, :rest] = vt[:, full * BLK:]
    for b in range(full):
        table[b * 32:(b + 1) * 32, :] = vt[:, b * BLK:(b + 1) * BLK]
    table[full * 32:(full + 1) * 32, :] = last[...]
    local = ids[...] - m * vt.shape[1]
    for p in range(4):
        mine = local[:, 256 * p:256 * (p + 1)]
        low = mine & (BLK - 1)
        high = mine >> 9
        spot = lax.broadcasted_iota(jnp.int32, (BLK, 256), 0)
        hot = jnp.where(spot == low, 1.0, 0.0).astype(BF16)
        looked = dot_n(table[...], hot)
        total = jnp.zeros((32, 256), F32)
        for b in range(full + 1):
            total = total + jnp.where(high == b, looked[b * 32:(b + 1) * 32, :], 0.0)
        for h in range(2):
            seq = 2 * p + h
            send[(seq // 2) * 4 + seq % 2, 32:64, :] = total[:, 128 * h:128 * (h + 1)]

    def project(basis, tokens, layer_at, first):
        out = dot_t(basis[...], tokens[...])
        for seq in range(8):
            send[(seq // 2) * 4 + 2 * layer_at + seq % 2, first:first + 32, :] = (
                out[:, 128 * seq:128 * (seq + 1)]
            )

    loads[3].wait()
    loads[4].wait()
    project(we, g0, 0, 0)
    loads[5].wait()
    loads[6].wait()
    project(wo, g1, 1, 0)
    loads[7].wait()
    loads[8].wait()
    project(wi, x1, 1, 32)
    loads[2].wait()
    loads[9].wait()
    qz[OWN] = jnp.concatenate([q[0].astype(F32), q[1].astype(F32)], axis=1).astype(BF16)

    pl.semaphore_wait(barrier, len(peers))

    for n, o in enumerate(z_offsets):
        go(remote(qz.at[OWN], qz.at[OWN - o], qz_send.at[n], qz_recv.at[n], along_z(o)))
    a_in = []
    for r in range(1, MS):
        there = (m + r) % MS
        copy = remote(send.at[there], recv.at[r - 1], a_send.at[r - 1], a_recv.at[r - 1], in_plane(r))
        go(copy)
        a_in.append(copy)

    def arrived_z(buffer, sems, n, o):
        remote(buffer.at[OWN], buffer.at[OWN - o], sems.at[n], sems.at[n], along_z(o)).wait_recv()

    for n, o in enumerate(z_offsets):
        arrived_z(qz, qz_recv, n, o)
    q_up = remote(qz.at[8:12], qz.at[12:16], qz_send.at[8], qz_recv.at[8], along_z(-REACH))
    q_down = remote(qz.at[4:7], qz.at[0:3], qz_send.at[9], qz_recv.at[9], along_z(REACH))
    go(q_up)
    go(q_down)

    for copy in a_in:
        copy.wait_recv()
    summed = send[m]
    for r in range(MS - 1):
        summed = summed + recv[r]
    lane8 = lax.broadcasted_iota(jnp.int32, (1, 8), 1)
    length = jnp.sum(jnp.where(lane8 == row, lens[...], 0), axis=1, keepdims=True)
    place = lax.broadcasted_iota(jnp.int32, (1, 128), 1)
    weight = jnp.where(place < length, 1.0 / length.astype(F32), 0.0)
    sk[...] = lax.dot_general(
        summed[:32] * weight, summed[32:], (((1,), (1,)), ((), ())),
        precision=lax.Precision.HIGHEST, preferred_element_type=F32,
    )
    sg[row, core, OWN] = jnp.concatenate(
        [sk[pl.ds(a, 8, stride=4), :] for a in range(4)], axis=1
    )

    def mine_of(lo, hi):
        return sg.at[row, core, lo:hi]

    own = sg.at[row, core]
    for n, o in enumerate(z_offsets):
        go(remote(own.at[OWN], own.at[OWN - o], sz_send.at[n], sz_recv.at[n], along_z(o)))

    q_up.wait_recv()
    q_down.wait_recv()
    for r in range(1, MS):
        go(remote(qz, qg.at[m, :, core], qp_send.at[r - 1], qp_recv.at[r - 1], in_plane(r)))
    go(remote(qz, qg.at[m, :, core], qs_send.at[0], qs_recv.at[0], sibling))
    for s in range(ZS):
        qg[m, s, core] = qz[s]

    for n, o in enumerate(z_offsets):
        arrived_z(own, sz_recv, n, o)
    s_up = remote(mine_of(8, 12), mine_of(12, 16), sz_send.at[8], sz_recv.at[8], along_z(-REACH))
    s_down = remote(mine_of(4, 7), mine_of(0, 3), sz_send.at[9], sz_recv.at[9], along_z(REACH))
    go(s_up)
    go(s_down)
    chunks = ((3, 12), (12, 16), (0, 3))

    def spread(k):
        lo, hi = chunks[k]
        for r in range(1, 8):
            go(remote(mine_of(lo, hi), mine_of(lo, hi), sp_send.at[k, r - 1], sp_recv.at[k, r - 1], in_group(r)))
        go(remote(mine_of(lo, hi), mine_of(lo, hi), ss_send.at[k, 0], ss_recv.at[k, 0], sibling))

    spread(0)

    for r in range(1, MS):
        origin = (m - r + MS) % MS
        block = qg.at[origin, :, core]
        remote(qz, block, qp_send.at[r - 1], qp_recv.at[r - 1], in_plane(r)).wait_recv()
        go(remote(block, block, qs_send.at[r], qs_recv.at[r], sibling))

    s_up.wait_recv()
    spread(1)
    s_down.wait_recv()
    spread(2)

    for r in range(MS):
        origin = (m - r + MS) % MS
        block = qg.at[origin, :, 1 - core]
        remote(block, block, qs_send.at[r], qs_recv.at[r], sibling).wait_recv()
    lane = lax.broadcasted_iota(jnp.int32, (16, 128), 1)
    left = lane < 64

    @pl.loop(0, ZS)
    def _(there):
        slot = (there - z + OWN + ZS) % ZS
        for s in range(8):
            a = qg[2 * s, slot].reshape(16, 128).astype(F32)
            b = qg[2 * s + 1, slot].reshape(16, 128).astype(F32)
            even = jnp.where(left, a, pltpu.roll(b, 64, 1))
            odd = jnp.where(left, pltpu.roll(a, 64, 1), b)
            both = jnp.where(layer == 0, even, odd)
            start = pl.multiple_of(there * 16, 16)
            bt[pl.ds(start, 16), 128 * s:128 * (s + 1)] = both.astype(BF16)

    square = bt[...].astype(F32)
    square_high, square_low = halves(square * square)
    ones = jnp.ones((8, 1024), BF16)
    bb[...] = dot_t(ones, square_high) + dot_t(ones, square_low)

    for k, (lo, hi) in enumerate(chunks):
        for r in range(1, 8):
            block = sg.at[(row - r + 8) % 8, core, lo:hi]
            remote(block, block, sp_send.at[k, r - 1], sp_recv.at[k, r - 1], in_group(r)).wait_recv()
            go(remote(block, block, ss_send.at[k, r], ss_recv.at[k, r], sibling))
    for k, (lo, hi) in enumerate(chunks):
        for r in range(8):
            block = sg.at[(row - r + 8) % 8, 1 - core, lo:hi]
            remote(block, block, ss_send.at[k, r], ss_recv.at[k, r], sibling).wait_recv()

    for i in range(8):
        for c in range(2):
            for s in range(8):
                piece = sg[i, c, :, s, :]
                ph, plow = halves(piece)
                at = (2 * i + c) * 16
                sh[at:at + 16, 128 * s:128 * (s + 1)] = ph
                sl[at:at + 16, 128 * s:128 * (s + 1)] = plow

    s_high, s_low = sh[...], sl[...]
    u = dot_t(s_high, bt[...]) + dot_t(s_low, bt[...])
    k_mat = dot_t(s_high, s_high) + dot_t(s_high, s_low) + dot_t(s_low, s_high)
    k_high, k_low = halves(k_mat)
    u_high, u_low = halves(u)
    v = dot_n(k_high, u_high) + dot_n(k_high, u_low) + dot_n(k_low, u_high)

    rr = bb[0:1, :]
    scaled = u * 0.0625
    uu = jnp.sum(scaled * scaled, axis=0, keepdims=True)
    step0 = rr / (uu + DAMPING * rr + EPSILON)
    keep = 1.0 - DAMPING * step0
    au = (step0 * 0.00390625) * u
    av = (step0 * 0.00390625) * v
    auu = step0 * uu
    aauv = jnp.sum(au * av, axis=0, keepdims=True)
    new = jnp.maximum(keep * keep * rr - 2.0 * keep * auu + aauv, 0.0)
    fac = keep + new / (rr + EPSILON)
    dd = jnp.maximum(fac * fac * rr - 2.0 * fac * auu + aauv, 0.0)
    y = fac * u - av
    scaled_y = y * 0.0625
    yy = jnp.sum(scaled_y * scaled_y, axis=0, keepdims=True)
    step1 = new / (yy + DAMPING * dd + EPSILON)
    scores = step0 * u + step1 * y
    parts0 = [scores[(2 * i) * 16 + OWN:(2 * i) * 16 + OWN + 1, :] for i in range(8)]
    parts1 = [scores[(2 * i + 1) * 16 + OWN:(2 * i + 1) * 16 + OWN + 1, :] for i in range(8)]
    part[...] = jnp.where(core == 0, jnp.concatenate(parts0, axis=0), jnp.concatenate(parts1, axis=0))

    final = remote(part, other, c_send.at[0], c_recv.at[0], partner)
    go(final)
    final.wait_recv()
    out_ref[...] = part[...] + other[...]
    for copy in sent:
        copy.wait_send()


def per_device(
    token_ids, lengths, embed_grads, vocab_basis, embed_basis,
    layer_inputs, layer_grads, input_basis, output_basis, queries,
):
    vocab = vocab_basis.shape[0]
    dma = pltpu.SemaphoreType.DMA
    return pl.pallas_call(
        kernel,
        out_shape=jax.ShapeDtypeStruct((8, 256), F32),
        in_specs=[pl.BlockSpec(memory_space=pl.ANY)] * 10,
        out_specs=pl.BlockSpec(memory_space=pltpu.VMEM),
        scratch_shapes=[
            pltpu.VMEM((1, 1024), jnp.int32),
            pltpu.VMEM((1, 8), jnp.int32),
            pltpu.VMEM((1024, 256), BF16),
            pltpu.VMEM((32, vocab), BF16),
            pltpu.VMEM((32, 256), BF16),
            pltpu.VMEM((1024, 256), BF16),
            pltpu.VMEM((1024, 256), BF16),
            pltpu.VMEM((32, 256), BF16),
            pltpu.VMEM((32, 256), BF16),
            pltpu.VMEM((2, 8, 64), BF16),
            pltpu.VMEM((32, BLK), BF16),
            pltpu.VMEM((512, BLK), BF16),
            pltpu.VMEM((MS, 64, 128), F32),
            pltpu.VMEM((MS - 1, 64, 128), F32),
            pltpu.VMEM((32, 32), F32),
            pltpu.VMEM((ZS, 8, 128), BF16),
            pltpu.VMEM((MS, ZS, 2, 8, 128), BF16),
            pltpu.VMEM((8, 2, ZS, 8, 128), F32),
            pltpu.VMEM((256, 1024), BF16),
            pltpu.VMEM((8, 256), F32),
            pltpu.VMEM((256, 1024), BF16),
            pltpu.VMEM((256, 1024), BF16),
            pltpu.VMEM((8, 256), F32),
            pltpu.VMEM((8, 256), F32),
            dma((10,)),
            dma((MS - 1,)), dma((MS - 1,)),
            dma((10,)), dma((10,)),
            dma((MS - 1,)), dma((MS - 1,)),
            dma((MS,)), dma((MS,)),
            dma((10,)), dma((10,)),
            dma((3, 7)), dma((3, 7)),
            dma((3, 8)), dma((3, 8)),
            dma((1,)), dma((1,)),
        ],
        compiler_params=pltpu.CompilerParams(
            collective_id=0, has_side_effects=True, vmem_limit_bytes=48 * 1024 * 1024
        ),
        name="attribution",
    )(
        token_ids.reshape(1, -1), lengths.reshape(1, -1), embed_grads, vocab_basis.T, embed_basis.T,
        layer_inputs[0], layer_grads[0], input_basis[0].T, output_basis[0].T,
        queries.transpose(0, 2, 1),
    )


def solution(mesh):
    placed = (
        P("dp"),
        P("dp"),
        P("dp", "mp"),
        P("mp", None),
        P("mp", None),
        P(None, "dp", "mp"),
        P(None, "dp", "mp"),
        P(None, "mp", None),
        P(None, "mp", None),
        P(None, "mp", "dp"),
    )
    return jax.shard_map(
        per_device, mesh=mesh, in_specs=placed, out_specs=P("dp", None), check_vma=False
    )
```

```python
import jax
import jax.numpy as jnp
from jax import lax
from jax.experimental import pallas as pl
from jax.experimental.pallas import tpu as pltpu
from jax.sharding import PartitionSpec as P

DAMPING = 0.01
EPSILON = 1e-06
MESH = pl.DeviceIdType.MESH
F32 = jnp.float32
BF16 = jnp.bfloat16

ZS = 16
MS = 16
REACH = 4
BLK = 512


def dot_t(a, b):
    return lax.dot_general(a, b, (((1,), (1,)), ((), ())), preferred_element_type=F32)


def dot_n(a, b):
    return lax.dot_general(a, b, (((1,), (0,)), ((), ())), preferred_element_type=F32)


def halves(a):
    high = a.astype(BF16)
    return high, (a - high.astype(F32)).astype(BF16)


def kernel(
    ids_hbm, len_hbm, g0_hbm, vt_hbm, we_hbm, x1_hbm, g1_hbm, wi_hbm, wo_hbm, q_hbm,
    out_ref,
    ids, lens, g0, vt, we, x1, g1, wi, wo, q,
    last, table, gsend, xsend, tsend, grecv, xrecv, trecv, xsum, sk,
    qz, qp, qg, sz, shl, bt, bb, part, other,
    in_sem, g_send, g_recv, x_send, x_recv, qz_send, qz_recv, qp_send, qp_recv, qs_send, qs_recv,
    sz_send, sz_recv, sp_send, sp_recv, ss_send, ss_recv, c_send, c_recv,
):
    d = lax.axis_index("dp")
    m = lax.axis_index("mp")
    core = d % 2
    z = d // 2
    x = m % 4
    layer = x // 2
    row = (m // 4) * 2 + x % 2
    sibling = (d + 1 - 2 * core, m)
    partner = (d, m - x + 3 - x)

    def along_z(offset):
        return (2 * ((z + offset + ZS) % ZS) + core, m)

    def in_plane(r):
        return (d, (m + r) % MS)

    def in_group(r):
        there = (row + r) % 8
        return (d, (there // 2) * 4 + 2 * layer + there % 2)

    pairs = [
        (q_hbm, q), (wo_hbm, wo), (g1_hbm, g1), (wi_hbm, wi), (x1_hbm, x1),
        (we_hbm, we), (g0_hbm, g0), (ids_hbm, ids), (vt_hbm, vt), (len_hbm, lens),
    ]
    loads = []
    for n, (src, dst) in enumerate(pairs):
        loads.append(pltpu.make_async_copy(src, dst, in_sem.at[n]))
        loads[n].start()

    barrier = pltpu.get_barrier_semaphore()
    z_offsets = [o for k in range(REACH, 0, -1) for o in (k, -k)]
    peers = [along_z(o) for o in z_offsets] + [in_plane(r) for r in range(1, MS)] + [sibling]
    for peer in peers:
        pl.semaphore_signal(barrier, inc=1, device_id=peer, device_id_type=MESH)

    def remote(src, dst, send_sem, recv_sem, peer):
        return pltpu.make_async_remote_copy(
            src_ref=src, dst_ref=dst, send_sem=send_sem, recv_sem=recv_sem,
            device_id=peer, device_id_type=MESH,
        )

    sent = []

    def go(copy):
        copy.start()
        sent.append(copy)

    def project(basis, tokens, layer_at, target):
        out = dot_t(basis[...], tokens[...])
        for seq in range(8):
            target[(seq // 2) * 4 + 2 * layer_at + seq % 2] = out[:, 128 * seq:128 * (seq + 1)]

    loads[0].wait()
    qz[z] = jnp.concatenate([q[0].astype(F32), q[1].astype(F32)], axis=1).astype(BF16)
    loads[1].wait()
    loads[2].wait()
    project(wo, g1, 1, gsend)
    loads[3].wait()
    loads[4].wait()
    project(wi, x1, 1, xsend)
    loads[5].wait()
    loads[6].wait()
    project(we, g0, 0, gsend)

    pl.semaphore_wait(barrier, len(peers))

    for n, o in enumerate(z_offsets):
        go(remote(qz.at[z], qz.at[z], qz_send.at[n], qz_recv.at[n], along_z(o)))
    g_in, x_in, t_in = [], [], []
    for r in range(1, MS):
        there = (m + r) % MS
        g_in.append(remote(gsend.at[there], grecv.at[r - 1], g_send.at[r - 1], g_recv.at[r - 1], in_plane(r)))
        x_in.append(remote(xsend.at[there], xrecv.at[r - 1], x_send.at[r - 1], x_recv.at[r - 1], in_plane(r)))
        t_in.append(remote(tsend.at[there], trecv.at[r - 1], x_send.at[r - 1], x_recv.at[r - 1], in_plane(r)))

    def layer_of(r):
        return ((m + r) % 4) // 2

    for r in range(1, MS):
        go(g_in[r - 1])

        @pl.when(layer_of(r) == 1)
        def _(r=r):
            x_in[r - 1].start()

    loads[7].wait()
    loads[8].wait()
    full = vt.shape[1] // BLK
    rest = vt.shape[1] - full * BLK
    last[...] = jnp.zeros(last.shape, BF16)
    last[:, :rest] = vt[:, full * BLK:]
    for b in range(full):
        table[b * 32:(b + 1) * 32, :] = vt[:, b * BLK:(b + 1) * BLK]
    table[full * 32:(full + 1) * 32, :] = last[...]
    local = ids[...] - m * vt.shape[1]
    for p in range(4):
        mine = local[:, 256 * p:256 * (p + 1)]
        low = mine & (BLK - 1)
        high = mine >> 9
        spot = lax.broadcasted_iota(jnp.int32, (BLK, 256), 0)
        hot = jnp.where(spot == low, 1.0, 0.0).astype(BF16)
        looked = dot_n(table[...], hot)
        total = jnp.zeros((32, 256), F32)
        for b in range(full + 1):
            total = total + jnp.where(high == b, looked[b * 32:(b + 1) * 32, :], 0.0)
        for h in range(2):
            seq = 2 * p + h
            tsend[(seq // 2) * 4 + seq % 2] = total[:, 128 * h:128 * (h + 1)].astype(BF16)
    for r in range(1, MS):
        @pl.when(layer_of(r) == 0)
        def _(r=r):
            t_in[r - 1].start()

    loads[9].wait()
    for n, o in enumerate(z_offsets):
        spot = qz.at[(z - o + ZS) % ZS]
        remote(spot, spot, qz_send.at[n], qz_recv.at[n], along_z(o)).wait_recv()
    legs = [(j, -REACH) for j in range(1, REACH + 1)] + [(-j, REACH) for j in range(1, REACH)]
    for n, (j, to) in enumerate(legs):
        spot = qz.at[(z + j + ZS) % ZS]
        go(remote(spot, spot, qz_send.at[8 + n], qz_recv.at[8 + n], along_z(to)))

    for copy in g_in:
        copy.wait_recv()

    @pl.when(layer == 1)
    def _():
        for copy in x_in:
            copy.wait_recv()
        total = xsend[m]
        for r in range(MS - 1):
            total = total + xrecv[r]
        xsum[...] = total

    @pl.when(layer == 0)
    def _():
        for copy in t_in:
            copy.wait_recv()
        total = tsend[m].astype(F32)
        for r in range(MS - 1):
            total = total + trecv[r].astype(F32)
        xsum[...] = total

    gsum = gsend[m]
    for r in range(MS - 1):
        gsum = gsum + grecv[r]
    lane8 = lax.broadcasted_iota(jnp.int32, (1, 8), 1)
    length = jnp.sum(jnp.where(lane8 == row, lens[...], 0), axis=1, keepdims=True)
    place = lax.broadcasted_iota(jnp.int32, (1, 128), 1)
    weight = jnp.where(place < length, 1.0 / length.astype(F32), 0.0)
    sk[...] = lax.dot_general(
        gsum * weight, xsum[...], (((1,), (1,)), ((), ())),
        precision=lax.Precision.HIGHEST, preferred_element_type=F32,
    )
    sz[4] = jnp.concatenate([sk[pl.ds(a, 8, stride=4), :] for a in range(4)], axis=1)

    def z_copy(t):
        slot = (4 - t) % ZS
        return remote(sz.at[4], sz.at[slot], sz_send.at[slot], sz_recv.at[slot], along_z(t))

    for t in [8] + [o for k in range(7, 0, -1) for o in (k, -k)]:
        go(z_copy(t))

    for n, (j, to) in enumerate(legs):
        spot = qz.at[(z - to + j + ZS) % ZS]
        remote(spot, spot, qz_send.at[8 + n], qz_recv.at[8 + n], along_z(to)).wait_recv()
    left = lax.broadcasted_iota(jnp.int32, (64, 128), 1) < 64
    first, second = qz[0:8].reshape(64, 128).astype(F32), qz[8:16].reshape(64, 128).astype(F32)
    qp[0] = jnp.where(left, first, pltpu.roll(second, 64, 1)).astype(BF16)
    qp[1] = jnp.where(left, pltpu.roll(first, 64, 1), second).astype(BF16)
    for r in range(1, MS):
        go(remote(qp.at[layer_of(r)], qg.at[m, core], qp_send.at[r - 1], qp_recv.at[r - 1], in_plane(r)))
    go(remote(qp.at[layer], qg.at[m, core], qs_send.at[0], qs_recv.at[0], sibling))
    qg[m, core] = qp[layer]

    def block_at(i, c, k):
        return shl.at[:, :, (2 * i + c) * 2 + k]

    def spread(k):
        for j in range(8 * k, 8 * k + 8):
            if j != 4:
                z_copy((4 - j) % ZS).wait_recv()
        for s in range(8):
            high, low = halves(sz[8 * k:8 * k + 8, s, :])
            shl[0, s, (2 * row + core) * 2 + k] = high
            shl[1, s, (2 * row + core) * 2 + k] = low
        block = block_at(row, core, k)
        for r in range(1, 8):
            go(remote(block, block, sp_send.at[k, r - 1], sp_recv.at[k, r - 1], in_group(r)))
        go(remote(block, block, ss_send.at[k, 0], ss_recv.at[k, 0], sibling))

    spread(0)

    for r in range(1, MS):
        block = qg.at[(m - r + MS) % MS, core]
        remote(qp.at[0], block, qp_send.at[r - 1], qp_recv.at[r - 1], in_plane(r)).wait_recv()
        go(remote(block, block, qs_send.at[r], qs_recv.at[r], sibling))

    spread(1)

    for r in range(MS):
        block = qg.at[(m - r + MS) % MS, 1 - core]
        remote(block, block, qs_send.at[r], qs_recv.at[r], sibling).wait_recv()
    for s in range(8):
        even, odd = [], []
        for c in range(2):
            a = qg[2 * s, c].astype(F32)
            b = qg[2 * s + 1, c].astype(F32)
            even.append(jnp.where(left, a, pltpu.roll(b, 64, 1)))
            odd.append(jnp.where(left, pltpu.roll(a, 64, 1), b))
        for h, both in enumerate((even, odd)):
            rows = [both[c][8 * k:8 * k + 8] for k in range(8) for c in range(2)]
            bt[128 * h:128 * h + 128, 128 * s:128 * (s + 1)] = jnp.concatenate(rows, axis=0).astype(BF16)

    square = bt[...].astype(F32)
    square_high, square_low = halves(square * square)
    ones = jnp.ones((8, 1024), BF16)
    bb[...] = dot_t(ones, square_high) + dot_t(ones, square_low)

    for k in range(2):
        for r in range(1, 8):
            block = block_at((row - r + 8) % 8, core, k)
            remote(block, block, sp_send.at[k, r - 1], sp_recv.at[k, r - 1], in_group(r)).wait_recv()
            go(remote(block, block, ss_send.at[k, r], ss_recv.at[k, r], sibling))
    for k in range(2):
        for r in range(8):
            block = block_at((row - r + 8) % 8, 1 - core, k)
            remote(block, block, ss_send.at[k, r], ss_recv.at[k, r], sibling).wait_recv()

    s_high = jnp.concatenate([shl[0, s].reshape(256, 128) for s in range(8)], axis=1)
    s_low = jnp.concatenate([shl[1, s].reshape(256, 128) for s in range(8)], axis=1)
    u = dot_t(s_high, bt[...]) + dot_t(s_low, bt[...])
    k_mat = dot_t(s_high, s_high) + dot_t(s_high, s_low) + dot_t(s_low, s_high)
    k_high, k_low = halves(k_mat)
    u_high, u_low = halves(u)
    v = dot_n(k_high, u_high) + dot_n(k_high, u_low) + dot_n(k_low, u_high)

    rr = bb[0:1, :]
    scaled = u * 0.0625
    uu = jnp.sum(scaled * scaled, axis=0, keepdims=True)
    step0 = rr / (uu + DAMPING * rr + EPSILON)
    keep = 1.0 - DAMPING * step0
    au = (step0 * 0.00390625) * u
    av = (step0 * 0.00390625) * v
    auu = step0 * uu
    aauv = jnp.sum(au * av, axis=0, keepdims=True)
    new = jnp.maximum(keep * keep * rr - 2.0 * keep * auu + aauv, 0.0)
    fac = keep + new / (rr + EPSILON)
    dd = jnp.maximum(fac * fac * rr - 2.0 * fac * auu + aauv, 0.0)
    y = fac * u - av
    scaled_y = y * 0.0625
    yy = jnp.sum(scaled_y * scaled_y, axis=0, keepdims=True)
    step1 = new / (yy + DAMPING * dd + EPSILON)
    scores = step0 * u + step1 * y
    rows = [
        jnp.concatenate([scores[32 * i + 16 * c + 4:32 * i + 16 * c + 5, :] for i in range(8)], axis=0)
        for c in range(2)
    ]
    part[...] = jnp.where(core == 0, rows[0], rows[1])

    final = remote(part, other, c_send.at[0], c_recv.at[0], partner)
    go(final)
    final.wait_recv()
    out_ref[...] = part[...] + other[...]
    for r in range(1, MS):
        @pl.when(layer_of(r) == 1)
        def _(r=r):
            x_in[r - 1].wait_send()

        @pl.when(layer_of(r) == 0)
        def _(r=r):
            t_in[r - 1].wait_send()
    for copy in sent:
        copy.wait_send()


def per_device(
    token_ids, lengths, embed_grads, vocab_basis, embed_basis,
    layer_inputs, layer_grads, input_basis, output_basis, queries,
):
    vocab = vocab_basis.shape[0]
    dma = pltpu.SemaphoreType.DMA
    return pl.pallas_call(
        kernel,
        out_shape=jax.ShapeDtypeStruct((8, 256), F32),
        in_specs=[pl.BlockSpec(memory_space=pl.ANY)] * 10,
        out_specs=pl.BlockSpec(memory_space=pltpu.VMEM),
        scratch_shapes=[
            pltpu.VMEM((1, 1024), jnp.int32),
            pltpu.VMEM((1, 8), jnp.int32),
            pltpu.VMEM((1024, 256), BF16),
            pltpu.VMEM((32, vocab), BF16),
            pltpu.VMEM((32, 256), BF16),
            pltpu.VMEM((1024, 256), BF16),
            pltpu.VMEM((1024, 256), BF16),
            pltpu.VMEM((32, 256), BF16),
            pltpu.VMEM((32, 256), BF16),
            pltpu.VMEM((2, 8, 64), BF16),
            pltpu.VMEM((32, BLK), BF16),
            pltpu.VMEM((512, BLK), BF16),
            pltpu.VMEM((MS, 32, 128), F32),
            pltpu.VMEM((MS, 32, 128), F32),
            pltpu.VMEM((MS, 32, 128), BF16),
            pltpu.VMEM((MS - 1, 32, 128), F32),
            pltpu.VMEM((MS - 1, 32, 128), F32),
            pltpu.VMEM((MS - 1, 32, 128), BF16),
            pltpu.VMEM((32, 128), F32),
            pltpu.VMEM((32, 32), F32),
            pltpu.VMEM((ZS, 8, 128), BF16),
            pltpu.VMEM((2, 64, 128), BF16),
            pltpu.VMEM((MS, 2, 64, 128), BF16),
            pltpu.VMEM((ZS, 8, 128), F32),
            pltpu.VMEM((2, 8, 32, 8, 128), BF16),
            pltpu.VMEM((256, 1024), BF16),
            pltpu.VMEM((8, 256), F32),
            pltpu.VMEM((8, 256), F32),
            pltpu.VMEM((8, 256), F32),
            dma((10,)),
            dma((MS - 1,)), dma((MS - 1,)), dma((MS - 1,)), dma((MS - 1,)),
            dma((15,)), dma((15,)),
            dma((MS - 1,)), dma((MS - 1,)),
            dma((MS,)), dma((MS,)),
            dma((ZS,)), dma((ZS,)),
            dma((2, 7)), dma((2, 7)),
            dma((2, 8)), dma((2, 8)),
            dma((1,)), dma((1,)),
        ],
        compiler_params=pltpu.CompilerParams(
            collective_id=0, has_side_effects=True
        ),
        name="attribution",
    )(
        token_ids.reshape(1, -1), lengths.reshape(1, -1), embed_grads, vocab_basis.T, embed_basis.T,
        layer_inputs[0], layer_grads[0], input_basis[0].T, output_basis[0].T,
        queries.transpose(0, 2, 1),
    )


def solution(mesh):
    placed = (
        P("dp"),
        P("dp"),
        P("dp", "mp"),
        P("mp", None),
        P("mp", None),
        P(None, "dp", "mp"),
        P(None, "dp", "mp"),
        P(None, "mp", None),
        P(None, "mp", None),
        P(None, "mp", "dp"),
    )
    return jax.shard_map(
        per_device, mesh=mesh, in_specs=placed, out_specs=P("dp", None), check_vma=False
    )
```

```python
import jax
import jax.numpy as jnp
from jax import lax
from jax.experimental import pallas as pl
from jax.experimental.pallas import tpu as pltpu
from jax.sharding import PartitionSpec as P

DAMPING = 0.01
EPSILON = 1e-06
MESH = pl.DeviceIdType.MESH
F32 = jnp.float32
BF16 = jnp.bfloat16

ZS = 16
MS = 16
REACH = 4
BLK = 512


def dot_t(a, b):
    return lax.dot_general(a, b, (((1,), (1,)), ((), ())), preferred_element_type=F32)


def dot_n(a, b):
    return lax.dot_general(a, b, (((1,), (0,)), ((), ())), preferred_element_type=F32)


def halves(a):
    high = a.astype(BF16)
    return high, (a - high.astype(F32)).astype(BF16)


def kernel(
    ids_hbm, len_hbm, g0_hbm, vt_hbm, we_hbm, x1_hbm, g1_hbm, wi_hbm, wo_hbm, q_hbm,
    out_ref,
    ids, lens, g0, vt, we, x1, g1, wi, wo, q,
    last, table, gsend, xsend, tsend, grecv, xrecv, trecv, xsum, sk,
    qz, qp, qg, sz, shl, bt, bb, part, other,
    in_sem, g_send, g_recv, x_send, t_send, x_recv, qz_send, qz_recv, qp_send, qp_recv, qs_send, qs_recv,
    sz_send, sz_recv, sp_send, sp_recv, ss_send, ss_recv, c_send, c_recv,
):
    d = lax.axis_index("dp")
    m = lax.axis_index("mp")
    core = d % 2
    z = d // 2
    x = m % 4
    y = m // 4
    layer = x // 2
    row = y * 2 + x % 2
    sibling = (d + 1 - 2 * core, m)
    partner = (d, m - x + 3 - x)

    def along_z(offset):
        return (2 * ((z + offset + ZS) % ZS) + core, m)

    def hops(k):
        return min(k, 4 - k)

    plane = sorted(((i, j) for i in range(4) for j in range(4) if i or j), key=lambda k: -hops(k[0]) - hops(k[1]))

    def there_of(i, j):
        return (y + j) % 4 * 4 + (x + i) % 4

    def layer_of(i):
        return (x + i) % 4 // 2

    group = sorted(((i, j) for i in range(2) for j in range(4) if i or j), key=lambda k: -k[0] - hops(k[1]))
    odd_x = x % 2

    def group_row(i, j):
        return (y + j + 4) % 4 * 2 + (odd_x + i) % 2

    def in_group(i, j):
        return (d, (y + j) % 4 * 4 + 2 * layer + (odd_x + i) % 2)

    pairs = [
        (q_hbm, q), (wo_hbm, wo), (g1_hbm, g1), (wi_hbm, wi), (x1_hbm, x1),
        (we_hbm, we), (g0_hbm, g0), (ids_hbm, ids), (vt_hbm, vt), (len_hbm, lens),
    ]
    loads = []
    for n, (src, dst) in enumerate(pairs):
        loads.append(pltpu.make_async_copy(src, dst, in_sem.at[n]))
        loads[n].start()

    barrier = pltpu.get_barrier_semaphore()
    z_offsets = [o for k in range(REACH, 0, -1) for o in (k, -k)]
    peers = [along_z(o) for o in z_offsets] + [(d, there_of(i, j)) for i, j in plane] + [sibling]
    for peer in peers:
        pl.semaphore_signal(barrier, inc=1, device_id=peer, device_id_type=MESH)

    def remote(src, dst, send_sem, recv_sem, peer):
        return pltpu.make_async_remote_copy(
            src_ref=src, dst_ref=dst, send_sem=send_sem, recv_sem=recv_sem,
            device_id=peer, device_id_type=MESH,
        )

    def take(sem, whole):
        remote(whole, whole, sem, sem, sibling).wait_recv()

    def drain(sem, whole):
        remote(whole, whole, sem, sem, sibling).wait_send()

    def project(basis, tokens, layer_at, target):
        out = dot_t(basis[...], tokens[...])
        for seq in range(8):
            target[(seq // 2) * 4 + 2 * layer_at + seq % 2] = out[:, 128 * seq:128 * (seq + 1)]

    loads[0].wait()
    qz[z] = jnp.concatenate([q[0].astype(F32), q[1].astype(F32)], axis=1).astype(BF16)
    loads[1].wait()
    loads[2].wait()
    project(wo, g1, 1, gsend)
    loads[3].wait()
    loads[4].wait()
    project(wi, x1, 1, xsend)
    loads[5].wait()
    loads[6].wait()
    project(we, g0, 0, gsend)

    pl.semaphore_wait(barrier, len(peers))

    for o in z_offsets:
        remote(qz.at[z], qz.at[z], qz_send.at[0], qz_recv.at[0], along_z(o)).start()
    for r, (i, j) in enumerate(plane):
        there = there_of(i, j)
        remote(gsend.at[there], grecv.at[r], g_send, g_recv, (d, there)).start()

        @pl.when(layer_of(i) == 1)
        def _(r=r, there=there):
            remote(xsend.at[there], xrecv.at[r], x_send, x_recv, (d, there)).start()

    loads[7].wait()
    loads[8].wait()
    full = vt.shape[1] // BLK
    rest = vt.shape[1] - full * BLK
    last[...] = jnp.zeros(last.shape, BF16)
    last[:, :rest] = vt[:, full * BLK:]
    for b in range(full):
        table[b * 32:(b + 1) * 32, :] = vt[:, b * BLK:(b + 1) * BLK]
    table[full * 32:(full + 1) * 32, :] = last[...]
    local = ids[...] - m * vt.shape[1]
    for p in range(4):
        mine = local[:, 256 * p:256 * (p + 1)]
        low = mine & (BLK - 1)
        high = mine >> 9
        spot = lax.broadcasted_iota(jnp.int32, (BLK, 256), 0)
        hot = jnp.where(spot == low, 1.0, 0.0).astype(BF16)
        looked = dot_n(table[...], hot)
        total = jnp.zeros((32, 256), F32)
        for b in range(full + 1):
            total = total + jnp.where(high == b, looked[b * 32:(b + 1) * 32, :], 0.0)
        for h in range(2):
            seq = 2 * p + h
            tsend[(seq // 2) * 4 + seq % 2] = total[:, 128 * h:128 * (h + 1)].astype(BF16)
    for r, (i, j) in enumerate(plane):
        there = there_of(i, j)

        @pl.when(layer_of(i) == 0)
        def _(r=r, there=there):
            remote(tsend.at[there], trecv.at[r], t_send, x_recv, (d, there)).start()

    loads[9].wait()
    take(qz_recv.at[0], qz.at[0:8])
    legs = [(k, -REACH) for k in range(1, REACH + 1)] + [(-k, REACH) for k in range(1, REACH)]
    for k, to in legs:
        spot = qz.at[(z + k + ZS) % ZS]
        remote(spot, spot, qz_send.at[1], qz_recv.at[1], along_z(to)).start()

    take(g_recv, grecv)

    @pl.when(layer == 1)
    def _():
        take(x_recv, xrecv)
        total = xsend[m]
        for r in range(MS - 1):
            total = total + xrecv[r]
        xsum[...] = total

    @pl.when(layer == 0)
    def _():
        take(x_recv, trecv)
        total = tsend[m].astype(F32)
        for r in range(MS - 1):
            total = total + trecv[r].astype(F32)
        xsum[...] = total

    gsum = gsend[m]
    for r in range(MS - 1):
        gsum = gsum + grecv[r]
    lane8 = lax.broadcasted_iota(jnp.int32, (1, 8), 1)
    length = jnp.sum(jnp.where(lane8 == row, lens[...], 0), axis=1, keepdims=True)
    place = lax.broadcasted_iota(jnp.int32, (1, 128), 1)
    weight = jnp.where(place < length, 1.0 / length.astype(F32), 0.0)
    sk[...] = lax.dot_general(
        gsum * weight, xsum[...], (((1,), (1,)), ((), ())),
        precision=lax.Precision.HIGHEST, preferred_element_type=F32,
    )
    sz[4] = jnp.concatenate([sk[pl.ds(a, 8, stride=4), :] for a in range(4)], axis=1)

    for t in [8] + [o for k in (1, 7, 2, 6, 3, 5, 4) for o in (k, -k)]:
        slot = (4 - t) % ZS
        remote(sz.at[4], sz.at[slot], sz_send, sz_recv.at[slot // 8], along_z(t)).start()

    take(qz_recv.at[1], qz.at[0:7])
    left = lax.broadcasted_iota(jnp.int32, (64, 128), 1) < 64
    first, second = qz[0:8].reshape(64, 128).astype(F32), qz[8:16].reshape(64, 128).astype(F32)
    qp[0] = jnp.where(left, first, pltpu.roll(second, 64, 1)).astype(BF16)
    qp[1] = jnp.where(left, pltpu.roll(first, 64, 1), second).astype(BF16)
    for i, j in plane:
        remote(qp.at[layer_of(i)], qg.at[m, core], qp_send, qp_recv, (d, there_of(i, j))).start()
    qg[m, core] = qp[layer]

    def block_at(i, c, k):
        return shl.at[:, :, (2 * i + c) * 2 + k]

    def spread(k):
        take(sz_recv.at[k], sz.at[0:7] if k == 0 else sz.at[0:8])
        for s in range(8):
            high, low = halves(sz[8 * k:8 * k + 8, s, :])
            shl[0, s, (2 * row + core) * 2 + k] = high
            shl[1, s, (2 * row + core) * 2 + k] = low
        block = block_at(row, core, k)
        for r, (i, j) in enumerate(group):
            remote(block, block, sp_send, sp_recv.at[k, r], in_group(i, j)).start()
        remote(block, block, ss_send, ss_recv.at[k], sibling).start()

    spread(0)

    take(qp_recv, qg.at[0:15, core])
    remote(qg.at[:, core], qg.at[:, core], qs_send, qs_recv, sibling).start()

    spread(1)

    take(qs_recv, qg.at[:, 1 - core])
    for s in range(8):
        even, odd = [], []
        for c in range(2):
            a = qg[2 * s, c].astype(F32)
            b = qg[2 * s + 1, c].astype(F32)
            even.append(jnp.where(left, a, pltpu.roll(b, 64, 1)))
            odd.append(jnp.where(left, pltpu.roll(a, 64, 1), b))
        for h, both in enumerate((even, odd)):
            rows = [both[c][8 * k:8 * k + 8] for k in range(8) for c in range(2)]
            bt[128 * h:128 * h + 128, 128 * s:128 * (s + 1)] = jnp.concatenate(rows, axis=0).astype(BF16)

    square = bt[...].astype(F32)
    square_high, square_low = halves(square * square)
    ones = jnp.ones((8, 1024), BF16)
    bb[...] = dot_t(ones, square_high) + dot_t(ones, square_low)

    for k in range(2):
        for r, (i, j) in enumerate(group):
            block = block_at(group_row(i, -j), core, k)
            take(sp_recv.at[k, r], block)
            remote(block, block, ss_send, ss_recv.at[k], sibling).start()
    for k in range(2):
        take(ss_recv.at[k], shl.at[:, :, 0:8])

    s_high = jnp.concatenate([shl[0, s].reshape(256, 128) for s in range(8)], axis=1)
    s_low = jnp.concatenate([shl[1, s].reshape(256, 128) for s in range(8)], axis=1)
    u = dot_t(s_high, bt[...]) + dot_t(s_low, bt[...])
    k_mat = dot_t(s_high, s_high) + dot_t(s_high, s_low) + dot_t(s_low, s_high)
    k_high, k_low = halves(k_mat)
    u_high, u_low = halves(u)
    v = dot_n(k_high, u_high) + dot_n(k_high, u_low) + dot_n(k_low, u_high)

    rr = bb[0:1, :]
    scaled = u * 0.0625
    uu = jnp.sum(scaled * scaled, axis=0, keepdims=True)
    step0 = rr / (uu + DAMPING * rr + EPSILON)
    keep = 1.0 - DAMPING * step0
    au = (step0 * 0.00390625) * u
    av = (step0 * 0.00390625) * v
    auu = step0 * uu
    aauv = jnp.sum(au * av, axis=0, keepdims=True)
    new = jnp.maximum(keep * keep * rr - 2.0 * keep * auu + aauv, 0.0)
    fac = keep + new / (rr + EPSILON)
    dd = jnp.maximum(fac * fac * rr - 2.0 * fac * auu + aauv, 0.0)
    y = fac * u - av
    scaled_y = y * 0.0625
    yy = jnp.sum(scaled_y * scaled_y, axis=0, keepdims=True)
    step1 = new / (yy + DAMPING * dd + EPSILON)
    scores = step0 * u + step1 * y
    rows = [
        jnp.concatenate([scores[32 * i + 16 * c + 4:32 * i + 16 * c + 5, :] for i in range(8)], axis=0)
        for c in range(2)
    ]
    part[...] = jnp.where(core == 0, rows[0], rows[1])

    final = remote(part, other, c_send, c_recv, partner)
    final.start()
    final.wait_recv()
    out_ref[...] = part[...] + other[...]
    final.wait_send()
    drain(qz_send.at[0], qz.at[0:8])
    drain(qz_send.at[1], qz.at[0:7])
    drain(g_send, grecv)
    drain(sz_send, sz.at[0:15])
    drain(qp_send, qg.at[0:15, core])
    drain(qs_send, qg.at[:, core])
    drain(sp_send, shl.at[:, :, 0:14])
    drain(ss_send, shl.at[:, :, 0:16])

    @pl.when(layer == 1)
    def _():
        drain(x_send, xsend.at[0:7])
        drain(t_send, tsend.at[0:8])

    @pl.when(layer == 0)
    def _():
        drain(x_send, xsend.at[0:8])
        drain(t_send, tsend.at[0:7])


def per_device(
    token_ids, lengths, embed_grads, vocab_basis, embed_basis,
    layer_inputs, layer_grads, input_basis, output_basis, queries,
):
    vocab = vocab_basis.shape[0]
    dma = pltpu.SemaphoreType.DMA
    return pl.pallas_call(
        kernel,
        out_shape=pltpu.VMEM((8, 256), F32),
        in_specs=[pl.BlockSpec(memory_space=pl.ANY)] * 10,
        out_specs=pl.BlockSpec(memory_space=pltpu.VMEM),
        scratch_shapes=[
            pltpu.VMEM((1, 1024), jnp.int32),
            pltpu.VMEM((1, 8), jnp.int32),
            pltpu.VMEM((1024, 256), BF16),
            pltpu.VMEM((32, vocab), BF16),
            pltpu.VMEM((32, 256), BF16),
            pltpu.VMEM((1024, 256), BF16),
            pltpu.VMEM((1024, 256), BF16),
            pltpu.VMEM((32, 256), BF16),
            pltpu.VMEM((32, 256), BF16),
            pltpu.VMEM((2, 8, 64), BF16),
            pltpu.VMEM((32, BLK), BF16),
            pltpu.VMEM((512, BLK), BF16),
            pltpu.VMEM((MS, 32, 128), F32),
            pltpu.VMEM((MS, 32, 128), F32),
            pltpu.VMEM((MS, 32, 128), BF16),
            pltpu.VMEM((MS - 1, 32, 128), F32),
            pltpu.VMEM((MS - 1, 32, 128), F32),
            pltpu.VMEM((MS - 1, 32, 128), BF16),
            pltpu.VMEM((32, 128), F32),
            pltpu.VMEM((32, 32), F32),
            pltpu.VMEM((ZS, 8, 128), BF16),
            pltpu.VMEM((2, 64, 128), BF16),
            pltpu.VMEM((MS, 2, 64, 128), BF16),
            pltpu.VMEM((ZS, 8, 128), F32),
            pltpu.VMEM((2, 8, 32, 8, 128), BF16),
            pltpu.VMEM((256, 1024), BF16),
            pltpu.VMEM((8, 256), F32),
            pltpu.VMEM((8, 256), F32),
            pltpu.VMEM((8, 256), F32),
            dma((10,)),
            dma, dma, dma, dma, dma,
            dma((2,)), dma((2,)),
            dma, dma, dma, dma,
            dma, dma((2,)),
            dma, dma((2, 7)),
            dma, dma((2,)),
            dma, dma,
        ],
        compiler_params=pltpu.CompilerParams(
            collective_id=0, has_side_effects=True
        ),
        name="attribution",
    )(
        token_ids.reshape(1, -1), lengths.reshape(1, -1), embed_grads, vocab_basis.T, embed_basis.T,
        layer_inputs[0], layer_grads[0], input_basis[0].T, output_basis[0].T,
        queries.transpose(0, 2, 1),
    )


def solution(mesh):
    placed = (
        P("dp"),
        P("dp"),
        P("dp", "mp"),
        P("mp", None),
        P("mp", None),
        P(None, "dp", "mp"),
        P(None, "dp", "mp"),
        P(None, "mp", None),
        P(None, "mp", None),
        P(None, "mp", "dp"),
    )
    return jax.shard_map(
        per_device, mesh=mesh, in_specs=placed, out_specs=P("dp", None), check_vma=False
    )
```
